32 devices in a mesh: dp: 4 (over x, y), tp: 8 (over z, core).
Axes of the slice: x: 2, y: 2, z: 4, core: 2. Of those that a mesh axis runs over, the one named last changes fastest.
Arguments:
- x: bfloat16 [8192, 5120], P('dp'), parts along dimension 0
- dy: bfloat16 [8192, 5120], P('dp'), parts along dimension 0
- gate: bfloat16 [8192, 14336], P('dp', 'tp'), parts along dimension 0
- up: bfloat16 [8192, 14336], P('dp', 'tp'), parts along dimension 0
- w_gate: bfloat16 [5120, 14336], P(None, 'tp')
- w_up: bfloat16 [5120, 14336], P(None, 'tp')
- w_down: bfloat16 [14336, 5120], P('tp')
Outputs:
- output 1: bfloat16 [8192, 5120], P('dp'), parts along dimension 0
- output 2: bfloat16 [20480, 14336], P('dp', 'tp'), parts along dimension 0
- output 3: bfloat16 [20480, 14336], P('dp', 'tp'), parts along dimension 0
- output 4: bfloat16 [57344, 5120], P(('dp', 'tp')), parts along dimension 0
There are 4 independent parts. The reference program is written for one: setup_inputs(seed, part) draws one part's arguments, and reference() takes and returns one part's arrays. A program takes and returns all parts, laid end to end along the dimension named above; an argument that names none is the same for every part.
All inputs are finite; a program needn't handle non-finite values.
Results may differ from the reference program's by a relative error of at most 0.012.
Values are sent between devices in bfloat16 or wider.
A program may use at most 2 GiB of HBM per device.

```python
import jax
import jax.numpy as jnp

ROWS = 2048
D = 5120
FF = 14336


def act(gate, up):
    return jax.nn.silu(gate) * up


def setup_inputs(seed: int = 0, part: int = 0) -> dict:
    kx, ky, ka, kb, kg, ku, kd = jax.random.split(jax.random.key(seed), 7)
    kx, ky, ka, kb = (jax.random.fold_in(k, part) for k in (kx, ky, ka, kb))
    drawn = {
        "x": jax.random.normal(kx, (ROWS, D), jnp.float32),
        "dy": jax.random.normal(ky, (ROWS, D), jnp.float32),
        "gate": jax.random.normal(ka, (ROWS, FF), jnp.float32),
        "up": jax.random.normal(kb, (ROWS, FF), jnp.float32),
        "w_gate": jax.random.normal(kg, (D, FF), jnp.float32) * D**-0.5,
        "w_up": jax.random.normal(ku, (D, FF), jnp.float32) * D**-0.5,
        "w_down": jax.random.normal(kd, (FF, D), jnp.float32) * FF**-0.5,
    }
    return {k: v.astype(jnp.bfloat16) for k, v in drawn.items()}


def reference(x, dy, gate, up, w_gate, w_up, w_down):
    hidden, back = jax.vjp(act, gate.astype(jnp.float32), up.astype(jnp.float32))
    d_hidden = jnp.dot(dy, w_down.T, preferred_element_type=jnp.float32)
    d_gate, d_up = (g.astype(jnp.bfloat16) for g in back(d_hidden))
    dx = jnp.dot(d_gate, w_gate.T, preferred_element_type=jnp.float32) + jnp.dot(d_up, w_up.T, preferred_element_type=jnp.float32)
    dw_gate = jnp.dot(x.T, d_gate, preferred_element_type=jnp.float32)
    dw_up = jnp.dot(x.T, d_up, preferred_element_type=jnp.float32)
    dw_down = jnp.dot(hidden.astype(jnp.bfloat16).T, dy, preferred_element_type=jnp.float32)
    return tuple(g.astype(jnp.bfloat16) for g in (dx, dw_gate, dw_up, dw_down))
```

```python
import functools

import jax
import jax.numpy as jnp
from jax import lax
from jax.experimental import pallas as pl
from jax.experimental.pallas import tpu as pltpu
from jax.sharding import PartitionSpec as P

BF, F32 = jnp.bfloat16, jnp.float32
MESH = pl.DeviceIdType.MESH
BLOCKS, JT, NT, XT = 4, 7, 10, 10
UNITS = BLOCKS * NT
RING, HOP = 8, 2


def dot(a, b, ca, cb):
    return lax.dot_general(a, b, (((ca,), (cb,)), ((), ())), preferred_element_type=F32)


def kernel(
    x, dy, gate, up, wg, wu, wd,
    dx, dwg, dwu, dwd, chip16, chip32,
    dg_all, du_all, hid_all, dyb, wdb, gb, ub, wgb, wub, xd, og, ou, od,
    tsend, xrecv, own, cst, abuf, bbuf, dbuf, fbuf, cfb,
    s_dy, s_wd, s_g, s_u, s_wg, s_wu, s_xd, s_og, s_ou, s_od,
    x_send, x_recv, s_c, s_cf, a_send, a_recv, b_send, b_recv, f_send, f_recv, p_send, p_recv, s_l,
):
    rb, cb = dyb.shape[0], wgb.shape[1]
    hb = rb // 2
    jb = wdb.shape[1]
    xb = xd.shape[2]
    ib = og.shape[1]
    t = lax.axis_index("tp")
    z, c = t // 2, lax.rem(t, 2)
    inner = jnp.logical_or(z == 1, z == 2)
    outer = jnp.logical_not(inner)
    partner = 2 * z + (1 - c)
    beside = 2 * (z + 1 - 2 * lax.rem(z, 2)) + c
    across = 2 * (3 - z) + c

    barrier = pltpu.get_barrier_semaphore()
    for to in (partner, beside):
        pl.semaphore_signal(barrier, inc=1, device_id={"tp": to}, device_id_type=MESH)

    @pl.when(inner)
    def _():
        pl.semaphore_signal(barrier, inc=1, device_id={"tp": across}, device_id_type=MESH)
        pl.semaphore_wait(barrier, 3)

    @pl.when(outer)
    def _():
        pl.semaphore_wait(barrier, 2)

    def local(src, dst, sem):
        return pltpu.make_async_copy(src, dst, sem)

    def remote(src, dst, send, recv, to):
        return pltpu.make_async_remote_copy(
            src_ref=src, dst_ref=dst, send_sem=send, recv_sem=recv, device_id={"tp": to}, device_id_type=MESH
        )

    def ds(i, n):
        return pl.ds(pl.multiple_of(i * n, n), n)

    def load_dy(b):
        return local(dy.at[ds(b, rb), :], dyb, s_dy)

    def load_hidden(g):
        b, j, s = g // JT, lax.rem(g, JT), lax.rem(g, 2)
        return (
            local(wd.at[ds(j, jb), :], wdb.at[s], s_wd.at[s]),
            local(gate.at[ds(b, rb), ds(j, jb)], gb.at[s], s_g.at[s]),
            local(up.at[ds(b, rb), ds(j, jb)], ub.at[s], s_u.at[s]),
        )

    def load_weights(u):
        n, s = lax.rem(u, NT), lax.rem(u, 2)
        return (
            local(wg.at[ds(n, cb), :], wgb.at[s], s_wg.at[s]),
            local(wu.at[ds(n, cb), :], wub.at[s], s_wu.at[s]),
        )

    def load_x(m, s):
        return local(x.at[:, ds(m, xb)], xd.at[s], s_xd.at[s])

    def load_dyt(m, s):
        return local(dy.at[:, ds(m, xb)], xd.at[s], s_xd.at[s])

    def start(copies):
        for copy in copies:
            copy.start()

    def wait(copies):
        for copy in copies:
            copy.wait()

    def part(u, half):
        b, n = u // NT, lax.rem(u, NT)
        return dx.at[ds(2 * b + half, hb), ds(n, cb)]

    def copy_x(u):
        s = lax.rem(u, 4)
        return remote(tsend.at[s], xrecv.at[s], x_send.at[s], x_recv.at[s], partner)

    def copy_c16(u):
        s = lax.rem(u, 2)
        return local(cst.at[s], chip16.at[u], s_c.at[s])

    def copy_c32(u):
        return local(own.at[lax.rem(u, 4)], chip32.at[u], s_c.at[lax.rem(u, 2)])

    def load_c32(u):
        s = lax.rem(u, 2)
        return local(chip32.at[u], cfb.at[s], s_cf.at[s])

    def copy_a(u):
        s = lax.rem(u, RING)
        return remote(chip16.at[u], abuf.at[s], a_send.at[s], a_recv.at[s], beside)

    def copy_b(u):
        s = lax.rem(u, RING)
        return remote(dbuf.at[s], bbuf.at[s], b_send.at[s], b_recv.at[s], across)

    def copy_f(u):
        return remote(fbuf.at[lax.rem(u, 4)], part(u, c), f_send.at[lax.rem(u, 4)], f_recv.at[u], beside)

    def copy_p_inner(u):
        return remote(fbuf.at[lax.rem(u, 4)], part(u, c), p_send.at[lax.rem(u, 4)], p_recv.at[u], partner)

    def copy_p_outer(u):
        return remote(part(u, c), part(u, c), p_send.at[lax.rem(u, 4)], p_recv.at[u], partner)

    def copy_l(u):
        return local(fbuf.at[lax.rem(u, 4)], part(u, c), s_l.at[lax.rem(u, 4)])

    def chip_sum(u):
        copy_x(u).wait_recv()
        s, o = lax.rem(u, 4), lax.rem(u, 4)
        total = own[o] + xrecv[s].astype(F32)

        @pl.when(outer)
        def _():
            cst[lax.rem(u, 2)] = total.astype(BF)
            copy_c16(u).start()

            @pl.when(u >= 1)
            def _():
                copy_c16(u - 1).wait()

        @pl.when(inner)
        def _():
            own[o] = total
            copy_c32(u).start()

            @pl.when(u >= 1)
            def _():
                copy_c32(u - 1).wait()

    def chip_sum_last():
        @pl.when(outer)
        def _():
            copy_c16(UNITS - 1).wait()

        @pl.when(inner)
        def _():
            copy_c32(UNITS - 1).wait()

    def valid(u):
        return jnp.logical_and(u >= 0, u < UNITS)

    def tick(s):
        @pl.when(outer)
        def _():
            v = s - 3 * HOP

            @pl.when(valid(v))
            def _():
                @pl.when(v >= 4)
                def _():
                    copy_p_outer(v - 4).wait_send()

                copy_f(v).wait_recv()
                copy_p_outer(v).start()

            @pl.when(valid(s))
            def _():
                @pl.when(s >= RING)
                def _():
                    copy_a(s - RING).wait_send()

                copy_a(s).start()

        @pl.when(inner)
        def _():
            w = s - HOP

            @pl.when(valid(w + 1))
            def _():
                load_c32(w + 1).start()

            v = s - 2 * HOP

            @pl.when(valid(v))
            def _():
                @pl.when(v >= 4)
                def _():
                    copy_f(v - 4).wait_send()
                    copy_p_inner(v - 4).wait_send()
                    copy_l(v - 4).wait()

                copy_b(v).wait_recv()
                r = lax.rem(v, RING)
                fbuf[lax.rem(v, 4)] = (dbuf[r].astype(F32) + bbuf[r].astype(F32)).astype(BF)
                copy_f(v).start()
                copy_p_inner(v).start()
                copy_l(v).start()
                copy_b(v).wait_send()

            @pl.when(valid(w))
            def _():
                r = lax.rem(w, RING)
                load_c32(w).wait()
                copy_a(w).wait_recv()
                dbuf[r] = (cfb[lax.rem(w, 2)] + abuf[r].astype(F32)).astype(BF)
                copy_b(w).start()

    zero = jnp.int32(0)
    load_dy(zero).start()
    start(load_hidden(zero))
    start(load_weights(zero))

    @pl.loop(0, BLOCKS)
    def _(b):
        load_dy(b).wait()
        rows = ds(b, rb)

        @pl.loop(0, JT)
        def _(j):
            g = b * JT + j
            s = lax.rem(g, 2)
            wait(load_hidden(g))

            @pl.when(g + 1 < BLOCKS * JT)
            def _():
                start(load_hidden(g + 1))

            dh = dot(dyb[...], wdb[s], 1, 1)
            gv, uv = gb[s].astype(F32), ub[s].astype(F32)
            sig = jax.nn.sigmoid(gv)
            silu = gv * sig
            cols = ds(j, jb)
            hid_all[rows, cols] = (silu * uv).astype(BF)
            du_all[rows, cols] = (dh * silu).astype(BF)
            dg_all[rows, cols] = (dh * uv * (sig + silu * (1.0 - sig))).astype(BF)

            @pl.when(jnp.logical_and(b >= 1, jnp.logical_or(j == 2, j == 5)))
            def _():
                tick(6 * b - 2 + (j >= 5).astype(jnp.int32))

        @pl.when(b + 1 < BLOCKS)
        def _():
            load_dy(b + 1).start()

        @pl.when(b + 1 == BLOCKS)
        def _():
            load_x(zero, zero).start()

        @pl.loop(0, NT)
        def _(n):
            u = b * NT + n
            s = lax.rem(u, 2)

            @pl.when(u >= 1)
            def _():
                chip_sum(u - 1)

            wait(load_weights(u))

            @pl.when(u + 1 < UNITS)
            def _():
                start(load_weights(u + 1))

            @pl.when(u >= 4)
            def _():
                copy_x(u - 4).wait_send()

            term = dot(dg_all[rows, :], wgb[s], 1, 1) + dot(du_all[rows, :], wub[s], 1, 1)
            o = lax.rem(u, 4)
            first, second = term[:hb], term[hb:]
            own[o] = jnp.where(c == 0, first, second)
            tsend[o] = jnp.where(c == 0, second, first).astype(BF)
            copy_x(u).start()

            here = functools.reduce(jnp.logical_or, [n == k for k in (2, 4, 7, 9)])

            @pl.when(here)
            def _():
                tick(6 * b + sum((n >= k).astype(jnp.int32) for k in (4, 7, 9)))

    last = jnp.int32(UNITS - 1)
    chip_sum(last)
    chip_sum_last()
    for k in range(UNITS - 4, UNITS):
        copy_x(jnp.int32(k)).wait_send()

    base = 6 * BLOCKS - 2

    def out_g(i):
        s = lax.rem(i, 2)
        return (
            local(og.at[s], dwg.at[ds(i, ib), :], s_og.at[s]),
            local(ou.at[s], dwu.at[ds(i, ib), :], s_ou.at[s]),
        )

    steps_x = 2 * XT

    @pl.loop(0, steps_x)
    def _(i):
        m, h = i // 2, lax.rem(i, 2)
        s = lax.rem(m, 2)

        @pl.when(h == 0)
        def _():
            load_x(m, s).wait()

            @pl.when(m + 1 < XT)
            def _():
                load_x(m + 1, 1 - s).start()

            @pl.when(m + 1 == XT)
            def _():
                load_dyt(zero, 1 - s).start()

        @pl.when(i >= 2)
        def _():
            wait(out_g(i - 2))

        xt = xd[s, :, ds(h, ib)]
        e = lax.rem(i, 2)
        og[e] = dot(xt, dg_all[...], 0, 0).astype(BF)
        ou[e] = dot(xt, du_all[...], 0, 0).astype(BF)
        start(out_g(i))

        @pl.when(lax.rem(i, 4) < 3)
        def _():
            tick(base + (i // 4) * 3 + lax.rem(i, 4))

    wait(out_g(jnp.int32(steps_x - 2)))
    wait(out_g(jnp.int32(steps_x - 1)))

    base2 = base + (steps_x // 4) * 3

    def out_d(k):
        s = lax.rem(k, 2)
        p, q = k // JT, lax.rem(k, JT)
        return local(od.at[s], dwd.at[ds(q, jb), ds(p, xb)], s_od.at[s])

    steps_d = XT * JT

    @pl.loop(0, steps_d)
    def _(k):
        p, q = k // JT, lax.rem(k, JT)
        s = lax.rem(p + XT, 2)

        @pl.when(q == 0)
        def _():
            load_dyt(p, s).wait()

            @pl.when(p + 1 < XT)
            def _():
                load_dyt(p + 1, 1 - s).start()

        @pl.when(k >= 2)
        def _():
            out_d(k - 2).wait()

        od[lax.rem(k, 2)] = dot(hid_all[:, ds(q, jb)], xd[s], 0, 0).astype(BF)
        out_d(k).start()

        @pl.when(lax.rem(k, 9) == 4)
        def _():
            tick(base2 + k // 9)

    out_d(jnp.int32(steps_d - 2)).wait()
    out_d(jnp.int32(steps_d - 1)).wait()

    done = base2 + steps_d // 9 + 1

    @pl.loop(done, UNITS + 3 * HOP)
    def _(s):
        tick(s)

    @pl.when(outer)
    def _():
        @pl.loop(UNITS - RING, UNITS)
        def _(u):
            copy_a(u).wait_send()

        @pl.loop(UNITS - 4, UNITS)
        def _(u):
            copy_p_outer(u).wait_send()

    @pl.when(inner)
    def _():
        @pl.loop(UNITS - 4, UNITS)
        def _(u):
            copy_f(u).wait_send()
            copy_p_inner(u).wait_send()
            copy_l(u).wait()

    @pl.loop(0, UNITS)
    def _(u):
        remote(part(u, 1 - c), part(u, 1 - c), p_send.at[0], p_recv.at[u], partner).wait_recv()


def solution(mesh):
    def step(x, dy, gate, up, w_gate, w_up, w_down):
        rows, d = x.shape
        f = gate.shape[1]
        rb, cb, jb, xb = rows // BLOCKS, d // NT, f // JT, d // XT
        hb, ib = rb // 2, xb // 2
        like = [jax.ShapeDtypeStruct(a.shape, a.dtype) for a in (x, w_gate, w_up, w_down)]
        like += [jax.ShapeDtypeStruct((UNITS, hb, cb), BF), jax.ShapeDtypeStruct((UNITS, hb, cb), F32)]
        dma = pltpu.SemaphoreType.DMA
        vm = pltpu.VMEM
        scratch = [
            vm((rows, f), BF), vm((rows, f), BF), vm((rows, f), BF),
            vm((rb, d), BF), vm((2, jb, d), BF), vm((2, rb, jb), BF), vm((2, rb, jb), BF),
            vm((2, cb, f), BF), vm((2, cb, f), BF), vm((2, rows, xb), BF),
            vm((2, ib, f), BF), vm((2, ib, f), BF), vm((2, jb, xb), BF),
            vm((4, hb, cb), BF), vm((4, hb, cb), BF), vm((4, hb, cb), F32), vm((2, hb, cb), BF),
            vm((RING, hb, cb), BF), vm((RING, hb, cb), BF), vm((RING, hb, cb), BF), vm((4, hb, cb), BF), vm((2, hb, cb), F32),
            dma(()), dma((2,)), dma((2,)), dma((2,)), dma((2,)), dma((2,)), dma((2,)), dma((2,)), dma((2,)), dma((2,)),
            dma((4,)), dma((4,)), dma((2,)), dma((2,)), dma((RING,)), dma((RING,)), dma((RING,)), dma((RING,)),
            dma((4,)), dma((UNITS,)), dma((4,)), dma((UNITS,)), dma((4,)),
        ]
        outs = pl.pallas_call(
            kernel,
            out_shape=like,
            in_specs=[pl.BlockSpec(memory_space=pl.ANY)] * 7,
            out_specs=[pl.BlockSpec(memory_space=pl.ANY)] * 6,
            scratch_shapes=scratch,
            compiler_params=pltpu.CompilerParams(
                collective_id=0, has_side_effects=True, vmem_limit_bytes=67_000_000
            ),
            name="mlp_backward",
        )(x, dy, gate, up, w_gate, w_up, w_down)
        return tuple(outs[:4])

    tokens, columns, rows = P("dp", None), P(None, "tp"), P("tp", None)
    return jax.shard_map(
        step,
        mesh=mesh,
        in_specs=(tokens, tokens, P("dp", "tp"), P("dp", "tp"), columns, columns, rows),
        out_specs=(tokens, P("dp", "tp"), P("dp", "tp"), P(("dp", "tp"), None)),
        check_vma=False,
    )
```

```python
import functools

import jax
import jax.numpy as jnp
from jax import lax
from jax.experimental import pallas as pl
from jax.experimental.pallas import tpu as pltpu
from jax.sharding import PartitionSpec as P

BF, F32 = jnp.bfloat16, jnp.float32
MESH = pl.DeviceIdType.MESH
BLOCKS, JT, NT, XT = 4, 7, 10, 10
UNITS = BLOCKS * NT
RING = 8
HALVES = 2 * (UNITS + 6)
CHUNKS, DT = 32, 5
AT_FIRST, AT_HIDDEN, AT_DX = (2, 3, 4, 5, 6, 7, 8, 9), (0, 1, 3, 4, 6), (0, 1, 2, 3, 4, 5, 6, 7, 8, 9)


def dot(a, b, ca, cb):
    return lax.dot_general(a, b, (((ca,), (cb,)), ((), ())), preferred_element_type=F32)


def kernel(
    x, dy, gate, up, wg, wu, wd,
    dx, dwg, dwu, hid, chip16, chip32,
    dg_all, du_all, hs, dyb, wdb, gb, ub, wgb, wub, xd, og, ou,
    tsend, xrecv, own, cst, abuf, bbuf, dbuf, fbuf, cfb,
    s_dy, s_wd, s_g, s_u, s_wg, s_wu, s_xd, s_og, s_ou, s_h,
    x_send, x_recv, s_c, s_cf, a_send, a_recv, b_send, b_recv, f_send, f_recv, p_send, p_recv, s_l,
):
    rb, cb = dyb.shape[0], wgb.shape[1]
    hb = rb // 2
    jb = wdb.shape[1]
    xb = xd.shape[2]
    ib = og.shape[1]
    t = lax.axis_index("tp")
    z, c = t // 2, lax.rem(t, 2)
    inner = jnp.logical_or(z == 1, z == 2)
    outer = jnp.logical_not(inner)
    partner = 2 * z + (1 - c)
    beside = 2 * (z + 1 - 2 * lax.rem(z, 2)) + c
    across = 2 * (3 - z) + c

    barrier = pltpu.get_barrier_semaphore()
    for to in (partner, beside):
        pl.semaphore_signal(barrier, inc=1, device_id={"tp": to}, device_id_type=MESH)

    @pl.when(inner)
    def _():
        pl.semaphore_signal(barrier, inc=1, device_id={"tp": across}, device_id_type=MESH)
        pl.semaphore_wait(barrier, 3)

    @pl.when(outer)
    def _():
        pl.semaphore_wait(barrier, 2)

    def local(src, dst, sem):
        return pltpu.make_async_copy(src, dst, sem)

    def remote(src, dst, send, recv, to):
        return pltpu.make_async_remote_copy(
            src_ref=src, dst_ref=dst, send_sem=send, recv_sem=recv, device_id={"tp": to}, device_id_type=MESH
        )

    def ds(i, n):
        return pl.ds(pl.multiple_of(i * n, n), n)

    def load_dy(b):
        return local(dy.at[ds(b, rb), :], dyb, s_dy)

    def load_hidden(g):
        b, j, s = g // JT, lax.rem(g, JT), lax.rem(g, 2)
        return (
            local(wd.at[ds(j, jb), :], wdb.at[s], s_wd.at[s]),
            local(gate.at[ds(b, rb), ds(j, jb)], gb.at[s], s_g.at[s]),
            local(up.at[ds(b, rb), ds(j, jb)], ub.at[s], s_u.at[s]),
        )

    def load_weights(u):
        n, s = lax.rem(u, NT), lax.rem(u, 2)
        return (
            local(wg.at[ds(n, cb), :], wgb.at[s], s_wg.at[s]),
            local(wu.at[ds(n, cb), :], wub.at[s], s_wu.at[s]),
        )

    def load_x(m, s):
        return local(x.at[:, ds(m, xb)], xd.at[s], s_xd.at[s])

    def start(copies):
        for copy in copies:
            copy.start()

    def wait(copies):
        for copy in copies:
            copy.wait()

    def part(u, half):
        b, n = u // NT, lax.rem(u, NT)
        return dx.at[ds(2 * b + half, hb), ds(n, cb)]

    def copy_x(u):
        s = lax.rem(u, 4)
        return remote(tsend.at[s], xrecv.at[s], x_send.at[s], x_recv.at[s], partner)

    def copy_c16(u):
        s = lax.rem(u, 2)
        return local(cst.at[s], chip16.at[u], s_c.at[s])

    def copy_c32(u):
        return local(own.at[lax.rem(u, 4)], chip32.at[u], s_c.at[lax.rem(u, 2)])

    def load_c32(u):
        s = lax.rem(u, 2)
        return local(chip32.at[u], cfb.at[s], s_cf.at[s])

    def copy_a(u):
        s = lax.rem(u, RING)
        return remote(chip16.at[u], abuf.at[s], a_send.at[s], a_recv.at[s], beside)

    def copy_b(u):
        s = lax.rem(u, RING)
        return remote(dbuf.at[s], bbuf.at[s], b_send.at[s], b_recv.at[s], across)

    def copy_f(u):
        return remote(fbuf.at[lax.rem(u, 4)], part(u, c), f_send.at[lax.rem(u, 4)], f_recv.at[u], beside)

    def copy_p_inner(u):
        return remote(fbuf.at[lax.rem(u, 4)], part(u, c), p_send.at[lax.rem(u, 4)], p_recv.at[u], partner)

    def copy_p_outer(u):
        return remote(part(u, c), part(u, c), p_send.at[lax.rem(u, 4)], p_recv.at[u], partner)

    def copy_l(u):
        return local(fbuf.at[lax.rem(u, 4)], part(u, c), s_l.at[lax.rem(u, 4)])

    def chip_sum(u):
        copy_x(u).wait_recv()
        s, o = lax.rem(u, 4), lax.rem(u, 4)
        total = own[o] + xrecv[s].astype(F32)

        @pl.when(outer)
        def _():
            cst[lax.rem(u, 2)] = total.astype(BF)
            copy_c16(u).start()

            @pl.when(u >= 1)
            def _():
                copy_c16(u - 1).wait()

        @pl.when(inner)
        def _():
            own[o] = total
            copy_c32(u).start()

            @pl.when(u >= 1)
            def _():
                copy_c32(u - 1).wait()

    def chip_sum_last():
        @pl.when(outer)
        def _():
            copy_c16(UNITS - 1).wait()

        @pl.when(inner)
        def _():
            copy_c32(UNITS - 1).wait()

    def valid(u):
        return jnp.logical_and(u >= 0, u < UNITS)

    def first_half(s):
        @pl.when(jnp.logical_and(outer, valid(s)))
        def _():
            @pl.when(s >= RING)
            def _():
                copy_a(s - RING).wait_send()

            copy_a(s).start()

        w = s - 2

        @pl.when(jnp.logical_and(inner, valid(w)))
        def _():
            r = lax.rem(w, RING)
            load_c32(w).wait()
            copy_a(w).wait_recv()
            dbuf[r] = (cfb[lax.rem(w, 2)] + abuf[r].astype(F32)).astype(BF)
            copy_b(w).start()

    def second_half(s):
        @pl.when(jnp.logical_and(inner, valid(s - 1)))
        def _():
            load_c32(s - 1).start()

        v = s - 4

        @pl.when(jnp.logical_and(inner, valid(v)))
        def _():
            @pl.when(v >= 4)
            def _():
                copy_f(v - 4).wait_send()
                copy_p_inner(v - 4).wait_send()
                copy_l(v - 4).wait()

            copy_b(v).wait_recv()
            r = lax.rem(v, RING)
            fbuf[lax.rem(v, 4)] = (dbuf[r].astype(F32) + bbuf[r].astype(F32)).astype(BF)
            copy_f(v).start()
            copy_p_inner(v).start()
            copy_l(v).start()
            copy_b(v).wait_send()

        q = s - 6

        @pl.when(jnp.logical_and(outer, valid(q)))
        def _():
            @pl.when(q >= 4)
            def _():
                copy_p_outer(q - 4).wait_send()

            copy_f(q).wait_recv()
            copy_p_outer(q).start()

    def half_step(h):
        @pl.when(lax.rem(h, 2) == 0)
        def _():
            first_half(h // 2)

        @pl.when(lax.rem(h, 2) == 1)
        def _():
            second_half(h // 2)

    def count(i, steps):
        return sum((i > k).astype(jnp.int32) for k in steps)

    def among(i, steps):
        return functools.reduce(jnp.logical_or, [i == k for k in steps])

    def out_h(g):
        b, j, s = g // JT, lax.rem(g, JT), lax.rem(g, 2)
        return local(hs.at[s], hid.at[ds(b, rb), ds(j, jb)], s_h.at[s])

    zero = jnp.int32(0)
    per_block = len(AT_HIDDEN) + len(AT_DX)
    load_dy(zero).start()
    start(load_hidden(zero))
    start(load_weights(zero))

    @pl.loop(0, BLOCKS)
    def _(b):
        load_dy(b).wait()
        rows = ds(b, rb)

        @pl.loop(0, JT)
        def _(j):
            g = b * JT + j
            s = lax.rem(g, 2)
            wait(load_hidden(g))

            @pl.when(g + 1 < BLOCKS * JT)
            def _():
                start(load_hidden(g + 1))

            dh = dot(dyb[...], wdb[s], 1, 1)
            gv, uv = gb[s].astype(F32), ub[s].astype(F32)
            sig = jax.nn.sigmoid(gv)
            silu = gv * sig
            cols = ds(j, jb)

            @pl.when(g >= 2)
            def _():
                out_h(g - 2).wait()

            hs[s] = (silu * uv).astype(BF)
            du_all[rows, cols] = (dh * silu).astype(BF)
            dg_all[rows, cols] = (dh * uv * (sig + silu * (1.0 - sig))).astype(BF)

            out_h(g).start()

            @pl.when(jnp.logical_and(b >= 1, among(j, AT_HIDDEN)))
            def _():
                half_step(len(AT_FIRST) + per_block * (b - 1) + count(j, AT_HIDDEN))

        @pl.when(b + 1 < BLOCKS)
        def _():
            load_dy(b + 1).start()

        @pl.when(b + 1 == BLOCKS)
        def _():
            load_x(zero, zero).start()

        @pl.loop(0, NT)
        def _(n):
            u = b * NT + n
            s = lax.rem(u, 2)

            wait(load_weights(u))

            @pl.when(u + 1 < UNITS)
            def _():
                start(load_weights(u + 1))

            @pl.when(u >= 4)
            def _():
                copy_x(u - 4).wait_send()

            term = dot(dg_all[rows, :], wgb[s], 1, 1) + dot(du_all[rows, :], wub[s], 1, 1)
            o = lax.rem(u, 4)
            first, second = term[:hb], term[hb:]
            own[o] = jnp.where(c == 0, first, second)
            tsend[o] = jnp.where(c == 0, second, first).astype(BF)
            copy_x(u).start()

            @pl.when(u >= 1)
            def _():
                chip_sum(u - 1)

            @pl.when(jnp.logical_and(b == 0, among(n, AT_FIRST)))
            def _():
                half_step(count(n, AT_FIRST))

            @pl.when(jnp.logical_and(b >= 1, among(n, AT_DX)))
            def _():
                half_step(len(AT_FIRST) + per_block * (b - 1) + len(AT_HIDDEN) + count(n, AT_DX))

    last = jnp.int32(UNITS - 1)
    chip_sum(last)
    chip_sum_last()
    for k in range(UNITS - 4, UNITS):
        copy_x(jnp.int32(k)).wait_send()

    out_h(jnp.int32(BLOCKS * JT - 2)).wait()
    out_h(jnp.int32(BLOCKS * JT - 1)).wait()
    base = len(AT_FIRST) + per_block * (BLOCKS - 1)

    def out_g(i):
        s = lax.rem(i, 2)
        return (
            local(og.at[s], dwg.at[ds(i, ib), :], s_og.at[s]),
            local(ou.at[s], dwu.at[ds(i, ib), :], s_ou.at[s]),
        )

    steps_x = 2 * XT

    @pl.loop(0, steps_x)
    def _(i):
        m, h = i // 2, lax.rem(i, 2)
        s = lax.rem(m, 2)

        @pl.when(h == 0)
        def _():
            load_x(m, s).wait()

            @pl.when(m + 1 < XT)
            def _():
                load_x(m + 1, 1 - s).start()

        @pl.when(i >= 2)
        def _():
            wait(out_g(i - 2))

        xt = xd[s, :, ds(h, ib)]
        e = lax.rem(i, 2)
        og[e] = dot(xt, dg_all[...], 0, 0).astype(BF)
        half_step(base + 2 * i)
        ou[e] = dot(xt, du_all[...], 0, 0).astype(BF)
        start(out_g(i))
        half_step(base + 2 * i + 1)

    wait(out_g(jnp.int32(steps_x - 2)))
    wait(out_g(jnp.int32(steps_x - 1)))

    @pl.loop(base + 2 * steps_x, HALVES)
    def _(h):
        half_step(h)

    @pl.when(outer)
    def _():
        @pl.loop(UNITS - RING, UNITS)
        def _(u):
            copy_a(u).wait_send()

        @pl.loop(UNITS - 4, UNITS)
        def _(u):
            copy_p_outer(u).wait_send()

    @pl.when(inner)
    def _():
        @pl.loop(UNITS - 4, UNITS)
        def _(u):
            copy_f(u).wait_send()
            copy_p_inner(u).wait_send()
            copy_l(u).wait()

    @pl.loop(0, UNITS)
    def _(u):
        remote(part(u, 1 - c), part(u, 1 - c), p_send.at[0], p_recv.at[u], partner).wait_recv()


def down_kernel(
    hid, dy, dx, dwg, dwu, dx_out, dwg_out, dwu_out, dwd, hv, xd, od, r0, r1, r2, s_h, s_xd, s_od, s_in, s_out
):
    jb, xb = hv.shape[2], xd.shape[2]
    moves = ((dx, dx_out, r0), (dwg, dwg_out, r1), (dwu, dwu_out, r2))
    steps = DT * JT

    def local(src, dst, sem):
        return pltpu.make_async_copy(src, dst, sem)

    def ds(i, n):
        return pl.ds(pl.multiple_of(i * n, n), n)

    def load_h(q):
        return local(hid.at[:, ds(q, jb)], hv.at[q], s_h.at[q])

    def load_dy(p):
        return local(dy.at[:, ds(p, xb)], xd.at[lax.rem(p, 2)], s_xd.at[lax.rem(p, 2)])

    def read(a, k):
        src, _, ring = moves[a]
        return local(src.at[ds(k, ring.shape[1]), :], ring.at[lax.rem(k, RING)], s_in.at[a, lax.rem(k, RING)])

    def write(a, k):
        _, dst, ring = moves[a]
        return local(ring.at[lax.rem(k, RING)], dst.at[ds(k, ring.shape[1]), :], s_out.at[a, lax.rem(k, RING)])

    def out_d(k):
        p, q, s = k // JT, lax.rem(k, JT), lax.rem(k, 2)
        return local(od.at[s], dwd.at[ds(q, jb), ds(p, xb)], s_od.at[s])

    load_dy(jnp.int32(0)).start()
    for q in range(JT):
        load_h(jnp.int32(q)).start()
        if q < 4:
            for a in range(3):
                read(a, jnp.int32(q)).start()

    @pl.loop(0, steps)
    def _(k):
        p, q = k // JT, lax.rem(k, JT)

        @pl.when(k < CHUNKS)
        def _():
            for a in range(3):
                read(a, k).wait()
                write(a, k).start()

                @pl.when(k >= 4)
                def _():
                    write(a, k - 4).wait()

                @pl.when(k + 4 < CHUNKS)
                def _():
                    read(a, k + 4).start()

        @pl.when(q == 0)
        def _():
            load_dy(p).wait()

            @pl.when(p + 1 < DT)
            def _():
                load_dy(p + 1).start()

        @pl.when(p == 0)
        def _():
            load_h(q).wait()

        @pl.when(k >= 2)
        def _():
            out_d(k - 2).wait()

        od[lax.rem(k, 2)] = dot(hv[q], xd[lax.rem(p, 2)], 0, 0).astype(BF)
        out_d(k).start()

    for k in (2, 1):
        out_d(jnp.int32(steps - k)).wait()
    for k in (4, 3, 2, 1):
        for a in range(3):
            write(a, jnp.int32(CHUNKS - k)).wait()


def solution(mesh):
    def step(x, dy, gate, up, w_gate, w_up, w_down):
        rows, d = x.shape
        f = gate.shape[1]
        rb, cb, jb, xb = rows // BLOCKS, d // NT, f // JT, d // XT
        hb, ib = rb // 2, xb // 2
        like = [jax.ShapeDtypeStruct(a.shape, a.dtype) for a in (x, w_gate, w_up, w_down)]
        between = [jax.ShapeDtypeStruct((rows, f), BF)]
        between += [jax.ShapeDtypeStruct((UNITS, hb, cb), BF), jax.ShapeDtypeStruct((UNITS, hb, cb), F32)]
        dma, vm = pltpu.SemaphoreType.DMA, pltpu.VMEM
        hbm = pl.BlockSpec(memory_space=pl.ANY)
        scratch = [
            vm((rows, f), BF), vm((rows, f), BF), vm((2, rb, jb), BF),
            vm((rb, d), BF), vm((2, jb, d), BF), vm((2, rb, jb), BF), vm((2, rb, jb), BF),
            vm((2, cb, f), BF), vm((2, cb, f), BF), vm((2, rows, xb), BF),
            vm((2, ib, f), BF), vm((2, ib, f), BF),
            vm((4, hb, cb), BF), vm((4, hb, cb), BF), vm((4, hb, cb), F32), vm((2, hb, cb), BF),
            vm((RING, hb, cb), BF), vm((RING, hb, cb), BF), vm((RING, hb, cb), BF), vm((4, hb, cb), BF), vm((2, hb, cb), F32),
            dma(()), dma((2,)), dma((2,)), dma((2,)), dma((2,)), dma((2,)), dma((2,)), dma((2,)), dma((2,)), dma((2,)),
            dma((4,)), dma((4,)), dma((2,)), dma((2,)), dma((RING,)), dma((RING,)), dma((RING,)), dma((RING,)),
            dma((4,)), dma((UNITS,)), dma((4,)), dma((UNITS,)), dma((4,)),
        ]
        dx, dwg, dwu, hid, *_ = pl.pallas_call(
            kernel,
            out_shape=like[:3] + between,
            in_specs=[hbm] * 7,
            out_specs=[hbm] * 6,
            scratch_shapes=scratch,
            compiler_params=pltpu.CompilerParams(
                collective_id=0, has_side_effects=True, vmem_limit_bytes=67_000_000
            ),
            name="mlp_backward",
        )(x, dy, gate, up, w_gate, w_up, w_down)
        return tuple(
            pl.pallas_call(
                down_kernel,
                out_shape=like,
                in_specs=[hbm] * 5,
                out_specs=[hbm] * 4,
                scratch_shapes=[
                    vm((JT, rows, jb), BF), vm((2, rows, d // DT), BF), vm((2, jb, d // DT), BF),
                    vm((RING, rows // CHUNKS, d), BF), vm((RING, d // CHUNKS, f), BF), vm((RING, d // CHUNKS, f), BF),
                    dma((JT,)), dma((2,)), dma((2,)), dma((3, RING)), dma((3, RING)),
                ],
                compiler_params=pltpu.CompilerParams(vmem_limit_bytes=67_000_000),
                name="mlp_down",
            )(hid, dy, dx, dwg, dwu)
        )

    tokens, columns, rows = P("dp", None), P(None, "tp"), P("tp", None)
    return jax.shard_map(
        step,
        mesh=mesh,
        in_specs=(tokens, tokens, P("dp", "tp"), P("dp", "tp"), columns, columns, rows),
        out_specs=(tokens, P("dp", "tp"), P("dp", "tp"), P(("dp", "tp"), None)),
        check_vma=False,
    )
```

```python
import functools

import jax
import jax.numpy as jnp
from jax import lax
from jax.experimental import pallas as pl
from jax.experimental.pallas import tpu as pltpu
from jax.sharding import PartitionSpec as P

BF, F32 = jnp.bfloat16, jnp.float32
MESH = pl.DeviceIdType.MESH
BLOCKS, JT, NT, XT = 4, 7, 10, 10
UNITS = BLOCKS * NT
RING = 8
HALVES = 2 * (UNITS + 6)
CHUNKS, DT = 32, 8
EARLY = 2
AT_FIRST, AT_HIDDEN, AT_DX = (2, 3, 4, 5, 6, 7, 8, 9), (0, 1, 3, 4, 6), (0, 1, 2, 3, 4, 5, 6, 7, 8, 9)


def dot(a, b, ca, cb):
    return lax.dot_general(a, b, (((ca,), (cb,)), ((), ())), preferred_element_type=F32)


def kernel(
    x, dy, gate, up, wg, wu, wd,
    dx, dwg, dwu, dwd, hid, chip16, chip32,
    dg_all, du_all, hid_early, od, hs, dyb, wdb, gb, ub, wgb, wub, xd, og, ou,
    tsend, xrecv, own, cst, abuf, bbuf, dbuf, fbuf, cfb,
    s_dy, s_wd, s_g, s_u, s_wg, s_wu, s_xd, s_og, s_ou, s_od, s_h,
    x_send, x_recv, s_c, s_cf, a_send, a_recv, b_send, b_recv, f_send, f_recv, p_send, p_recv, s_l,
):
    rb, cb = dyb.shape[0], wgb.shape[1]
    hb = rb // 2
    jb = wdb.shape[1]
    xb = xd.shape[2]
    ib = og.shape[1]
    t = lax.axis_index("tp")
    z, c = t // 2, lax.rem(t, 2)
    inner = jnp.logical_or(z == 1, z == 2)
    outer = jnp.logical_not(inner)
    partner = 2 * z + (1 - c)
    beside = 2 * (z + 1 - 2 * lax.rem(z, 2)) + c
    across = 2 * (3 - z) + c

    barrier = pltpu.get_barrier_semaphore()
    for to in (partner, beside):
        pl.semaphore_signal(barrier, inc=1, device_id={"tp": to}, device_id_type=MESH)

    @pl.when(inner)
    def _():
        pl.semaphore_signal(barrier, inc=1, device_id={"tp": across}, device_id_type=MESH)
        pl.semaphore_wait(barrier, 3)

    @pl.when(outer)
    def _():
        pl.semaphore_wait(barrier, 2)

    def local(src, dst, sem):
        return pltpu.make_async_copy(src, dst, sem)

    def remote(src, dst, send, recv, to):
        return pltpu.make_async_remote_copy(
            src_ref=src, dst_ref=dst, send_sem=send, recv_sem=recv, device_id={"tp": to}, device_id_type=MESH
        )

    def ds(i, n):
        return pl.ds(pl.multiple_of(i * n, n), n)

    def load_dy(b):
        return local(dy.at[ds(b, rb), :], dyb, s_dy)

    def load_hidden(g):
        b, j, s = g // JT, lax.rem(g, JT), lax.rem(g, 2)
        return (
            local(wd.at[ds(j, jb), :], wdb.at[s], s_wd.at[s]),
            local(gate.at[ds(b, rb), ds(j, jb)], gb.at[s], s_g.at[s]),
            local(up.at[ds(b, rb), ds(j, jb)], ub.at[s], s_u.at[s]),
        )

    def load_weights(u):
        n, s = lax.rem(u, NT), lax.rem(u, 2)
        return (
            local(wg.at[ds(n, cb), :], wgb.at[s], s_wg.at[s]),
            local(wu.at[ds(n, cb), :], wub.at[s], s_wu.at[s]),
        )

    def load_x(m, s):
        return local(x.at[:, ds(m, xb)], xd.at[s], s_xd.at[s])

    def load_dyt(m, s):
        return local(dy.at[:, ds(m, xb)], xd.at[s], s_xd.at[s])

    def start(copies):
        for copy in copies:
            copy.start()

    def wait(copies):
        for copy in copies:
            copy.wait()

    def part(u, half):
        b, n = u // NT, lax.rem(u, NT)
        return dx.at[ds(2 * b + half, hb), ds(n, cb)]

    def copy_x(u):
        s = lax.rem(u, 4)
        return remote(tsend.at[s], xrecv.at[s], x_send.at[s], x_recv.at[s], partner)

    def copy_c16(u):
        s = lax.rem(u, 2)
        return local(cst.at[s], chip16.at[u], s_c.at[s])

    def copy_c32(u):
        return local(own.at[lax.rem(u, 4)], chip32.at[u], s_c.at[lax.rem(u, 2)])

    def load_c32(u):
        s = lax.rem(u, 2)
        return local(chip32.at[u], cfb.at[s], s_cf.at[s])

    def copy_a(u):
        s = lax.rem(u, RING)
        return remote(chip16.at[u], abuf.at[s], a_send.at[s], a_recv.at[s], beside)

    def copy_b(u):
        s = lax.rem(u, RING)
        return remote(dbuf.at[s], bbuf.at[s], b_send.at[s], b_recv.at[s], across)

    def copy_f(u):
        return remote(fbuf.at[lax.rem(u, 4)], part(u, c), f_send.at[lax.rem(u, 4)], f_recv.at[u], beside)

    def copy_p_inner(u):
        return remote(fbuf.at[lax.rem(u, 4)], part(u, c), p_send.at[lax.rem(u, 4)], p_recv.at[u], partner)

    def copy_p_outer(u):
        return remote(part(u, c), part(u, c), p_send.at[lax.rem(u, 4)], p_recv.at[u], partner)

    def copy_l(u):
        return local(fbuf.at[lax.rem(u, 4)], part(u, c), s_l.at[lax.rem(u, 4)])

    def chip_sum(u):
        copy_x(u).wait_recv()
        s, o = lax.rem(u, 4), lax.rem(u, 4)
        total = own[o] + xrecv[s].astype(F32)

        @pl.when(outer)
        def _():
            cst[lax.rem(u, 2)] = total.astype(BF)
            copy_c16(u).start()

            @pl.when(u >= 1)
            def _():
                copy_c16(u - 1).wait()

        @pl.when(inner)
        def _():
            own[o] = total
            copy_c32(u).start()

            @pl.when(u >= 1)
            def _():
                copy_c32(u - 1).wait()

    def chip_sum_last():
        @pl.when(outer)
        def _():
            copy_c16(UNITS - 1).wait()

        @pl.when(inner)
        def _():
            copy_c32(UNITS - 1).wait()

    def valid(u):
        return jnp.logical_and(u >= 0, u < UNITS)

    def first_half(s):
        @pl.when(jnp.logical_and(outer, valid(s)))
        def _():
            @pl.when(s >= RING)
            def _():
                copy_a(s - RING).wait_send()

            copy_a(s).start()

        w = s - 2

        @pl.when(jnp.logical_and(inner, valid(w)))
        def _():
            r = lax.rem(w, RING)
            load_c32(w).wait()
            copy_a(w).wait_recv()
            dbuf[r] = (cfb[lax.rem(w, 2)] + abuf[r].astype(F32)).astype(BF)
            copy_b(w).start()

    def second_half(s):
        @pl.when(jnp.logical_and(inner, valid(s - 1)))
        def _():
            load_c32(s - 1).start()

        v = s - 4

        @pl.when(jnp.logical_and(inner, valid(v)))
        def _():
            @pl.when(v >= 4)
            def _():
                copy_f(v - 4).wait_send()
                copy_p_inner(v - 4).wait_send()
                copy_l(v - 4).wait()

            copy_b(v).wait_recv()
            r = lax.rem(v, RING)
            fbuf[lax.rem(v, 4)] = (dbuf[r].astype(F32) + bbuf[r].astype(F32)).astype(BF)
            copy_f(v).start()
            copy_p_inner(v).start()
            copy_l(v).start()
            copy_b(v).wait_send()

        q = s - 6

        @pl.when(jnp.logical_and(outer, valid(q)))
        def _():
            @pl.when(q >= 4)
            def _():
                copy_p_outer(q - 4).wait_send()

            copy_f(q).wait_recv()
            copy_p_outer(q).start()

    def half_step(h):
        @pl.when(lax.rem(h, 2) == 0)
        def _():
            first_half(h // 2)

        @pl.when(lax.rem(h, 2) == 1)
        def _():
            second_half(h // 2)

    def count(i, steps):
        return sum((i > k).astype(jnp.int32) for k in steps)

    def among(i, steps):
        return functools.reduce(jnp.logical_or, [i == k for k in steps])

    def out_h(g):
        b, j, s = g // JT, lax.rem(g, JT), lax.rem(g, 2)
        return local(hs.at[s], hid.at[ds(b, rb), ds(j, jb)], s_h.at[s])

    zero = jnp.int32(0)
    per_block = len(AT_HIDDEN) + len(AT_DX)
    load_dy(zero).start()
    start(load_hidden(zero))
    start(load_weights(zero))

    @pl.loop(0, BLOCKS)
    def _(b):
        load_dy(b).wait()
        rows = ds(b, rb)

        @pl.loop(0, JT)
        def _(j):
            g = b * JT + j
            s = lax.rem(g, 2)
            wait(load_hidden(g))

            @pl.when(g + 1 < BLOCKS * JT)
            def _():
                start(load_hidden(g + 1))

            dh = dot(dyb[...], wdb[s], 1, 1)
            gv, uv = gb[s].astype(F32), ub[s].astype(F32)
            sig = jax.nn.sigmoid(gv)
            silu = gv * sig
            cols = ds(j, jb)

            @pl.when(g >= 2)
            def _():
                out_h(g - 2).wait()

            hs[s] = (silu * uv).astype(BF)

            @pl.when(j < EARLY)
            def _():
                hid_early[rows, cols] = hs[s]

            du_all[rows, cols] = (dh * silu).astype(BF)
            dg_all[rows, cols] = (dh * uv * (sig + silu * (1.0 - sig))).astype(BF)

            out_h(g).start()

            @pl.when(jnp.logical_and(b >= 1, among(j, AT_HIDDEN)))
            def _():
                half_step(len(AT_FIRST) + per_block * (b - 1) + count(j, AT_HIDDEN))

        @pl.when(b + 1 < BLOCKS)
        def _():
            load_dy(b + 1).start()

        @pl.when(b + 1 == BLOCKS)
        def _():
            load_x(zero, zero).start()

        @pl.loop(0, NT)
        def _(n):
            u = b * NT + n
            s = lax.rem(u, 2)

            wait(load_weights(u))

            @pl.when(u + 1 < UNITS)
            def _():
                start(load_weights(u + 1))

            @pl.when(u >= 4)
            def _():
                copy_x(u - 4).wait_send()

            term = dot(dg_all[rows, :], wgb[s], 1, 1) + dot(du_all[rows, :], wub[s], 1, 1)
            o = lax.rem(u, 4)
            first, second = term[:hb], term[hb:]
            own[o] = jnp.where(c == 0, first, second)
            tsend[o] = jnp.where(c == 0, second, first).astype(BF)
            copy_x(u).start()

            @pl.when(u >= 1)
            def _():
                chip_sum(u - 1)

            @pl.when(jnp.logical_and(b == 0, among(n, AT_FIRST)))
            def _():
                half_step(count(n, AT_FIRST))

            @pl.when(jnp.logical_and(b >= 1, among(n, AT_DX)))
            def _():
                half_step(len(AT_FIRST) + per_block * (b - 1) + len(AT_HIDDEN) + count(n, AT_DX))

    last = jnp.int32(UNITS - 1)
    chip_sum(last)
    chip_sum_last()
    for k in range(UNITS - 4, UNITS):
        copy_x(jnp.int32(k)).wait_send()

    out_h(jnp.int32(BLOCKS * JT - 2)).wait()
    out_h(jnp.int32(BLOCKS * JT - 1)).wait()
    base = len(AT_FIRST) + per_block * (BLOCKS - 1)

    def out_g(i):
        s = lax.rem(i, 2)
        return (
            local(og.at[s], dwg.at[ds(i, ib), :], s_og.at[s]),
            local(ou.at[s], dwu.at[ds(i, ib), :], s_ou.at[s]),
        )

    steps_x = 2 * XT

    @pl.loop(0, steps_x)
    def _(i):
        m, h = i // 2, lax.rem(i, 2)
        s = lax.rem(m, 2)

        @pl.when(h == 0)
        def _():
            load_x(m, s).wait()

            @pl.when(m + 1 < XT)
            def _():
                load_x(m + 1, 1 - s).start()

            @pl.when(m + 1 == XT)
            def _():
                load_dyt(zero, 1 - s).start()

        @pl.when(i >= 2)
        def _():
            wait(out_g(i - 2))

        xt = xd[s, :, ds(h, ib)]
        e = lax.rem(i, 2)
        og[e] = dot(xt, dg_all[...], 0, 0).astype(BF)
        half_step(base + 3 * (i // 2) + 2 * h)
        ou[e] = dot(xt, du_all[...], 0, 0).astype(BF)
        start(out_g(i))

        @pl.when(h == 0)
        def _():
            half_step(base + 3 * (i // 2) + 1)

    wait(out_g(jnp.int32(steps_x - 2)))
    wait(out_g(jnp.int32(steps_x - 1)))

    base2 = base + 3 * XT

    def out_d(k):
        p, q, s = k // EARLY, lax.rem(k, EARLY), lax.rem(k, 2)
        return local(od.at[s], dwd.at[ds(q, jb), ds(p, xb)], s_od.at[s])

    steps_d = XT * EARLY

    @pl.loop(0, steps_d)
    def _(k):
        p, q = k // EARLY, lax.rem(k, EARLY)
        s = lax.rem(p + XT, 2)

        @pl.when(q == 0)
        def _():
            load_dyt(p, s).wait()

            @pl.when(p + 1 < XT)
            def _():
                load_dyt(p + 1, 1 - s).start()

        @pl.when(k >= 2)
        def _():
            out_d(k - 2).wait()

        od[lax.rem(k, 2)] = dot(hid_early[:, ds(q, jb)], xd[s], 0, 0).astype(BF)
        out_d(k).start()

        @pl.when(q == 0)
        def _():
            half_step(base2 + p)

    out_d(jnp.int32(steps_d - 2)).wait()
    out_d(jnp.int32(steps_d - 1)).wait()

    @pl.loop(base2 + XT, HALVES)
    def _(h):
        half_step(h)

    @pl.when(outer)
    def _():
        @pl.loop(UNITS - RING, UNITS)
        def _(u):
            copy_a(u).wait_send()

        @pl.loop(UNITS - 4, UNITS)
        def _(u):
            copy_p_outer(u).wait_send()

    @pl.when(inner)
    def _():
        @pl.loop(UNITS - 4, UNITS)
        def _(u):
            copy_f(u).wait_send()
            copy_p_inner(u).wait_send()
            copy_l(u).wait()

    @pl.loop(0, UNITS)
    def _(u):
        remote(part(u, 1 - c), part(u, 1 - c), p_send.at[0], p_recv.at[u], partner).wait_recv()


def down_kernel(
    hid, dy, dx, dwg, dwu, early, dx_out, dwg_out, dwu_out, dwd, hv, xd, od, r0, r1, r2, r3, s_h, s_xd, s_od, s_in, s_out
):
    jb, xb = hv.shape[2], xd.shape[2]
    moves = ((dx, dx_out, r0), (dwg, dwg_out, r1), (dwu, dwu_out, r2), (early, dwd, r3))
    late = JT - EARLY
    steps = DT * late

    def local(src, dst, sem):
        return pltpu.make_async_copy(src, dst, sem)

    def ds(i, n):
        return pl.ds(pl.multiple_of(i * n, n), n)

    def load_h(q):
        return local(hid.at[:, ds(q + EARLY, jb)], hv.at[q], s_h.at[q])

    def load_dy(p):
        return local(dy.at[:, ds(p, xb)], xd.at[lax.rem(p, 2)], s_xd.at[lax.rem(p, 2)])

    def read(a, k):
        src, _, ring = moves[a]
        return local(src.at[ds(k, ring.shape[1]), :], ring.at[lax.rem(k, RING)], s_in.at[a, lax.rem(k, RING)])

    def write(a, k):
        _, dst, ring = moves[a]
        return local(ring.at[lax.rem(k, RING)], dst.at[ds(k, ring.shape[1]), :], s_out.at[a, lax.rem(k, RING)])

    def out_d(k):
        p, q, s = k // late, lax.rem(k, late), lax.rem(k, 2)
        return local(od.at[s], dwd.at[ds(q + EARLY, jb), ds(p, xb)], s_od.at[s])

    load_dy(jnp.int32(0)).start()
    for q in range(late):
        load_h(jnp.int32(q)).start()
        if q < 4:
            for a in range(4):
                read(a, jnp.int32(q)).start()

    @pl.loop(0, steps)
    def _(k):
        p, q = k // late, lax.rem(k, late)

        @pl.when(k < CHUNKS)
        def _():
            for a in range(4):
                read(a, k).wait()
                write(a, k).start()

                @pl.when(k >= 4)
                def _():
                    write(a, k - 4).wait()

                @pl.when(k + 4 < CHUNKS)
                def _():
                    read(a, k + 4).start()

        @pl.when(q == 0)
        def _():
            load_dy(p).wait()

            @pl.when(p + 1 < DT)
            def _():
                load_dy(p + 1).start()

        @pl.when(p == 0)
        def _():
            load_h(q).wait()

        @pl.when(k >= 2)
        def _():
            out_d(k - 2).wait()

        od[lax.rem(k, 2)] = dot(hv[q], xd[lax.rem(p, 2)], 0, 0).astype(BF)
        out_d(k).start()

    for k in (2, 1):
        out_d(jnp.int32(steps - k)).wait()
    for k in (4, 3, 2, 1):
        for a in range(4):
            write(a, jnp.int32(CHUNKS - k)).wait()


def solution(mesh):
    def step(x, dy, gate, up, w_gate, w_up, w_down):
        rows, d = x.shape
        f = gate.shape[1]
        rb, cb, jb, xb = rows // BLOCKS, d // NT, f // JT, d // XT
        hb, ib = rb // 2, xb // 2
        like = [jax.ShapeDtypeStruct(a.shape, a.dtype) for a in (x, w_gate, w_up, w_down)]
        between = [jax.ShapeDtypeStruct((EARLY * jb, d), BF), jax.ShapeDtypeStruct((rows, f), BF)]
        between += [jax.ShapeDtypeStruct((UNITS, hb, cb), BF), jax.ShapeDtypeStruct((UNITS, hb, cb), F32)]
        dma, vm = pltpu.SemaphoreType.DMA, pltpu.VMEM
        hbm = pl.BlockSpec(memory_space=pl.ANY)
        scratch = [
            vm((rows, f), BF), vm((rows, f), BF), vm((rows, EARLY * jb), BF), vm((2, jb, xb), BF), vm((2, rb, jb), BF),
            vm((rb, d), BF), vm((2, jb, d), BF), vm((2, rb, jb), BF), vm((2, rb, jb), BF),
            vm((2, cb, f), BF), vm((2, cb, f), BF), vm((2, rows, xb), BF),
            vm((2, ib, f), BF), vm((2, ib, f), BF),
            vm((4, hb, cb), BF), vm((4, hb, cb), BF), vm((4, hb, cb), F32), vm((2, hb, cb), BF),
            vm((RING, hb, cb), BF), vm((RING, hb, cb), BF), vm((RING, hb, cb), BF), vm((4, hb, cb), BF), vm((2, hb, cb), F32),
            dma(()), dma((2,)), dma((2,)), dma((2,)), dma((2,)), dma((2,)), dma((2,)), dma((2,)), dma((2,)), dma((2,)), dma((2,)),
            dma((4,)), dma((4,)), dma((2,)), dma((2,)), dma((RING,)), dma((RING,)), dma((RING,)), dma((RING,)),
            dma((4,)), dma((UNITS,)), dma((4,)), dma((UNITS,)), dma((4,)),
        ]
        dx, dwg, dwu, early, hid, *_ = pl.pallas_call(
            kernel,
            out_shape=like[:3] + between,
            in_specs=[hbm] * 7,
            out_specs=[hbm] * 7,
            scratch_shapes=scratch,
            compiler_params=pltpu.CompilerParams(
                collective_id=0, has_side_effects=True, vmem_limit_bytes=67_000_000
            ),
            name="mlp_backward",
        )(x, dy, gate, up, w_gate, w_up, w_down)
        return tuple(
            pl.pallas_call(
                down_kernel,
                out_shape=like,
                in_specs=[hbm] * 6,
                out_specs=[hbm] * 4,
                scratch_shapes=[
                    vm((JT - EARLY, rows, jb), BF), vm((2, rows, d // DT), BF), vm((2, jb, d // DT), BF),
                    vm((RING, rows // CHUNKS, d), BF), vm((RING, d // CHUNKS, f), BF), vm((RING, d // CHUNKS, f), BF),
                    vm((RING, EARLY * jb // CHUNKS, d), BF),
                    dma((JT - EARLY,)), dma((2,)), dma((2,)), dma((4, RING)), dma((4, RING)),
                ],
                compiler_params=pltpu.CompilerParams(vmem_limit_bytes=67_000_000),
                name="mlp_down",
            )(hid, dy, dx, dwg, dwu, early)
        )

    tokens, columns, rows = P("dp", None), P(None, "tp"), P("tp", None)
    return jax.shard_map(
        step,
        mesh=mesh,
        in_specs=(tokens, tokens, P("dp", "tp"), P("dp", "tp"), columns, columns, rows),
        out_specs=(tokens, P("dp", "tp"), P("dp", "tp"), P(("dp", "tp"), None)),
        check_vma=False,
    )
```
